32 devices in a mesh: dp: 4 (over x, core), expert: 8 (over z, y).
Axes of the slice: x: 2, y: 2, z: 4, core: 2. Of those that a mesh axis runs over, the one named last changes fastest.
Arguments:
- tokens: bfloat16 [32768, 768], P(('dp', 'expert')), may hold values from -6 to 6
- lengths: int32 [32, 4], P(('dp', 'expert')), may hold values from 1 to 512, 1024 in all within a row
- routes: int32 [32768, 2], P(('dp', 'expert')), may hold values from 0 to 9, all different within a row; in each aligned block of 1024 rows (0 to 1023, 1024 to 2047, ...) at most 307 rows name the same one
- gain_one: float32 [768], replicated, may hold values from 0.5 to 1.5
- w_query: bfloat16 [768, 768], replicated, may hold values from -0.21875 to 0.21875
- w_key: bfloat16 [768, 768], replicated, may hold values from -0.21875 to 0.21875
- w_value: bfloat16 [768, 768], replicated, may hold values from -0.21875 to 0.21875
- w_attn_out: bfloat16 [768, 768], replicated, may hold values from -0.875 to 0.875
- gain_two: float32 [768], replicated, may hold values from 0.5 to 1.5
- w_gate: float32 [768, 10], replicated, may hold values from -0.15625 to 0.15625
- frozen_in: bfloat16 [2, 3072, 768], replicated, may hold values from -0.21875 to 0.21875
- frozen_out: bfloat16 [2, 3072, 768], replicated, may hold values from -0.15625 to 0.15625
- new_in: bfloat16 [8, 3072, 768], P('expert', 'dp'), may hold values from -0.21875 to 0.21875
- new_out: bfloat16 [8, 3072, 768], P('expert', 'dp'), may hold values from -0.15625 to 0.15625
- out_grad: bfloat16 [32768, 768], P(('dp', 'expert')), may hold values from -6 to 6
Outputs:
- output: bfloat16 [32768, 768], P(('dp', 'expert'))
- x_grad: float32 [32768, 768], P(('dp', 'expert'))
- gain_one_grad: float32 [768], replicated
- w_query_grad: float32 [768, 768], replicated
- w_key_grad: float32 [768, 768], replicated
- w_value_grad: float32 [768, 768], replicated
- w_attn_out_grad: float32 [768, 768], replicated
- gain_two_grad: float32 [768], replicated
- w_gate_grad: float32 [768, 10], replicated
- new_in_grad: float32 [8, 3072, 768], P('expert', 'dp')
- new_out_grad: float32 [8, 3072, 768], P('expert', 'dp')
The draws below stay inside these ranges and needn't reach their ends.
Inputs may be any that keep to these rules, and one draw needn't show every extreme that they name: `routes`: each row names two different experts; among the 1024 rows of one sequence no expert is named more than 307 times, a bound that some block reaches; every expert is named somewhere. Each row holds the lengths of 4 documents in order; they sum to 1024, the longest is exactly 512.
All inputs are finite; a program needn't handle non-finite values.
Results may differ from the reference program's by a relative error of at most 0.013.
Values may be sent and summed in bfloat16 or wider, within the bound.
A program may use at most 320 MiB of HBM per device.

```python
import math
from functools import partial
import jax
import jax.numpy as jnp
import numpy as np
from jax import lax

HEADS = 12
HEAD_DIM = 64
D = 768
FF = 3072
FROZEN = 2
DOCS = 4
SEQ = 1024
SEQS = 32
TOKENS = 32768
NEW = 8
EXPERTS = 10
CAP = 307


def levels(key, dims, pieces, smallest, top_value):
    def one(position, parts):
        heights = jax.random.uniform(jax.random.fold_in(jax.random.fold_in(key, 6), position), (parts,), jnp.float32, smallest / len(pieces), top_value / len(pieces))
        return jnp.repeat(jnp.exp(heights), dims[position] // parts).reshape((-1,) + (1,) * (len(dims) - position - 1))

    level = one(*pieces[0])
    for cut in pieces[1:]:
        level = level * one(*cut)
    return level


def split_up(number_of, total, bound, skew):
    loads = [(1 << 20) // math.isqrt(grade ** skew) + 1 for grade in range(2, number_of + 1)]
    surplus, holding = total - bound - (number_of - 1), [1] * (number_of - 1)
    while surplus > 0:
        candidates = [i for i in range(number_of - 1) if holding[i] < bound]
        whole, budget = sum([loads[i] for i in candidates]), surplus
        for i in candidates:
            addition = min(bound - holding[i], max(1, budget * loads[i] // whole), surplus)
            holding[i] = holding[i] + addition
            surplus = surplus - addition
    return np.array([bound] + holding)


def ragged(own_key, number_of, total, reach, skew):
    if number_of == 2:
        one = jax.random.randint(own_key, (), max(1, total - reach), min(reach, total - 1) + 1)
        return jnp.stack([one, total - one])
    sizes = jnp.asarray(split_up(number_of, total, reach, skew), jnp.int32)
    twos = (number_of - 1) // 2
    donor, receiver = sizes[1:1 + 2 * twos:2], sizes[2:2 + 2 * twos:2]
    margin = jnp.minimum(donor - 1, reach - receiver)
    moved = jax.random.randint(jax.random.fold_in(own_key, 1), (twos,), 0, 1 << 20) % (margin + 1)
    sizes = sizes.at[1:1 + 2 * twos:2].set(donor - moved).at[2:2 + 2 * twos:2].set(receiver + moved)
    return sizes[jax.random.permutation(jax.random.fold_in(own_key, 2), number_of)]


def deal_out(key, own, number, rows, amount, top, limit, skew):
    order = jax.random.permutation(key, amount)
    heavy_load, ordinary = load_shares(amount, rows * top, limit, skew, True), load_shares(amount, rows * top, limit, skew, False)
    places = jnp.arange(amount)

    def named(sizes, rotation):
        used = int((sizes > 0).sum())
        fixed = max(1, used // 4)
        shifted = fixed + (places - fixed + rotation * (used - fixed)) % max(1, amount - fixed)
        return jnp.zeros((amount,), jnp.int32).at[order[jnp.where(places < fixed, places, shifted)]].set(jnp.asarray(sizes, jnp.int32))

    sizes = jnp.where(number % 4 == 0, named(heavy_load, number // 4), named(ordinary, number - number // 4 - 1))
    mixed = jax.random.permutation(jax.random.fold_in(own, 3), amount)
    giver, sink = mixed[0:amount // 2 * 2:2], mixed[1:amount // 2 * 2:2]
    slack = jnp.minimum(sizes[giver] - 1, limit - sizes[sink]) // 2
    slack = jnp.where((giver == order[0]) | (sink == order[0]) | (sizes[sink] == 0), 0, jnp.maximum(slack, 0))
    shifted = jax.random.randint(jax.random.fold_in(own, 4), (amount // 2,), 0, 1 << 20) % (slack + 1)
    sizes = sizes.at[giver].add(-shifted).at[sink].add(shifted)
    labels = jnp.searchsorted(jnp.cumsum(sizes), jnp.arange(rows * top), side="right").astype(jnp.int32)
    grid = labels.reshape(top, rows).T
    grid = grid[jax.random.permutation(jax.random.fold_in(own, 1), rows)]
    rotation = jax.random.randint(jax.random.fold_in(own, 2), (rows, 1), 0, top)
    return jnp.take_along_axis(grid, (jnp.arange(top)[None, :] + rotation) % top, axis=1)


def load_shares(amount, total, bound, skew, full):
    weights = [(1 << 20) // math.isqrt(standing ** skew) + 1 for standing in range(1, amount + 1)]
    largest = bound if full else min(bound, max(-(-total // amount), total * weights[0] // sum(weights)))
    least = 1 if total - largest >= amount - 1 else 0
    given, spare = [largest] + [least] * (amount - 1), total - largest - least * (amount - 1)
    while spare > 0:
        movable = [i for i in range(1, amount) if given[i] < largest] or [i for i in range(1, amount) if given[i] < bound]
        mass, left = sum([weights[i] for i in movable]), spare
        for i in movable:
            more = min(bound - given[i], max(1, left * weights[i] // mass), spare)
            given[i] = given[i] + more
            spare = spare - more
    return np.array(given)


def scatter_about(stream_key, shape, scale, most, shards=(), held_as=jnp.bfloat16):
    array = scale * jax.random.normal(stream_key, shape, jnp.float32)
    if shards:
        array = array * levels(stream_key, shape, shards, -0.22, 0.18)
    return jnp.clip(array, -most, most).astype(held_as)


def setup_inputs(seed: int = 0) -> dict:
    key_of = jax.random.split(jax.random.key(seed), 16)
    tokens = scatter_about(key_of[0], (TOKENS, D), 1.0, 6.0, ((0, 32),))
    lengths = jax.vmap(lambda own: ragged(own, DOCS, SEQ, SEQ // 2, 1))(jax.random.split(key_of[1], SEQS)).reshape((SEQS, DOCS)).astype(jnp.int32)
    routes_keys = jax.random.split(jax.random.fold_in(key_of[2], 1), TOKENS // SEQ)
    routes_turns = jax.random.permutation(jax.random.fold_in(key_of[2], 3), TOKENS // SEQ)
    routes = jax.vmap(lambda own, number: deal_out(jax.random.fold_in(key_of[2], 2), own, number, SEQ, EXPERTS, 2, CAP, 1))(routes_keys, routes_turns).reshape((TOKENS, 2))
    gain_one = jnp.clip(1.0 + 0.1 * jax.random.normal(key_of[3], (D,), jnp.float32), 0.5, 1.5)
    w_query = scatter_about(key_of[4], (D, D), D ** -0.5, 0.21875)
    w_key = scatter_about(key_of[5], (D, D), D ** -0.5, 0.21875)
    w_value = scatter_about(key_of[6], (D, D), D ** -0.5, 0.21875)
    w_attn_out = scatter_about(key_of[7], (D, D), (D // 16) ** -0.5, 0.875)
    gain_two = jnp.clip(1.0 + 0.1 * jax.random.normal(key_of[8], (D,), jnp.float32), 0.5, 1.5)
    w_gate = scatter_about(key_of[9], (D, EXPERTS), (2 * D) ** -0.5, 0.15625, (), jnp.float32)
    frozen_in = scatter_about(key_of[10], (FROZEN, FF, D), D ** -0.5, 0.21875)
    frozen_out = scatter_about(key_of[11], (FROZEN, FF, D), (FF // 2) ** -0.5, 0.15625)
    new_in = scatter_about(key_of[12], (NEW, FF, D), D ** -0.5, 0.21875, ((0, 8), (1, 4)))
    new_out = scatter_about(key_of[13], (NEW, FF, D), (FF // 2) ** -0.5, 0.15625, ((0, 8), (1, 4)))
    out_grad = scatter_about(key_of[14], (TOKENS, D), 1.0, 6.0, ((0, 32),))
    return {"tokens": tokens, "lengths": lengths, "routes": routes, "gain_one": gain_one, "w_query": w_query, "w_key": w_key, "w_value": w_value, "w_attn_out": w_attn_out, "gain_two": gain_two, "w_gate": w_gate, "frozen_in": frozen_in, "frozen_out": frozen_out, "new_in": new_in, "new_out": new_out, "out_grad": out_grad}


@jax.custom_vjp
def low(v):
    return lax.optimization_barrier(v.astype(jnp.bfloat16)).astype(jnp.float32)

@jax.custom_vjp
def low_back(v):
    return v

def low_keep(v):
    return (low(v), None)

def low_pass(kept, grad):
    return (grad,)

def back_keep(v):
    return (v, None)

def back_low(kept, grad):
    return (low(grad),)
low.defvjp(low_keep, low_pass)
low_back.defvjp(back_keep, back_low)
highest = lax.Precision.HIGHEST
epsilon = 1e-05
masked_score = -1000000000.0

def layer_norm(inputs, gain):
    centre = inputs - lax.optimization_barrier(jnp.mean(inputs, axis=-1, keepdims=True))
    return centre * lax.rsqrt(lax.optimization_barrier(jnp.mean(centre * centre, axis=-1, keepdims=True)) + epsilon) * gain

def doc_ids(length_row, seq_len):
    ends = jnp.cumsum(length_row).astype(jnp.int32)
    places = jnp.arange(seq_len, dtype=jnp.int32)
    return lax.optimization_barrier(jnp.sum((places[:, None] >= ends[None, :]).astype(jnp.int32), axis=1)).astype(jnp.int32)

def slot_tables(route_row, experts, capacity, seq_len):
    flat = route_row.reshape(-1).astype(jnp.int32)
    picks = (flat[:, None] == jnp.arange(experts, dtype=jnp.int32)[None, :]).astype(jnp.int32)
    ranks = lax.optimization_barrier(jnp.sum((jnp.cumsum(picks, axis=0).astype(jnp.int32) - 1) * picks, axis=1)).astype(jnp.int32)
    spots = (flat * capacity + ranks).astype(jnp.int32)
    owners = jnp.full((experts * capacity,), 2 * seq_len, jnp.int32)
    owners = owners.at[spots].set(jnp.arange(2 * seq_len, dtype=jnp.int32))
    return (spots, owners)

def front_block(x_row, length_row, route_row, owner_row, gain_one, w_query, w_key, w_value, w_attn_out, gain_two, w_gate):
    split_shape = (SEQ, HEADS, HEAD_DIM)
    normed = low(layer_norm(x_row, gain_one))
    query = low(low_back(jnp.dot(normed, w_query, precision=highest))).reshape(split_shape)
    keys = low(low_back(jnp.dot(normed, w_key, precision=highest))).reshape(split_shape)
    values = low(low_back(jnp.dot(normed, w_value, precision=highest))).reshape(split_shape)
    scores = low_back(jnp.einsum('qhd,khd->hqk', query, keys, precision=highest) * HEAD_DIM ** (-0.5))
    doc = doc_ids(length_row, SEQ)
    places = jnp.arange(SEQ, dtype=jnp.int32)
    allowed = (doc[:, None] == doc[None, :]) & (places[None, :] <= places[:, None])
    scores = jnp.where(allowed[None], scores, masked_score)
    top = lax.optimization_barrier(jnp.max(scores, axis=-1, keepdims=True))
    expd = jnp.exp(scores - top)
    probs = expd / lax.optimization_barrier(jnp.sum(expd, axis=-1, keepdims=True))
    mixed = jnp.einsum('hqk,khd->qhd', low(probs), values, precision=highest)
    mixed = low(low_back(mixed.reshape(SEQ, D)))
    hidden = x_row + low_back(jnp.dot(mixed, w_attn_out, precision=highest))
    normed_two = layer_norm(hidden, gain_two)
    logits = jnp.dot(normed_two, w_gate, precision=highest)
    picks = (route_row[:, :, None] == jnp.arange(EXPERTS, dtype=jnp.int32)[None, None, :]).astype(jnp.float32)
    chosen = jnp.einsum('te,tke->tk', logits, picks, precision=highest)
    weights = jnp.exp(chosen - lax.optimization_barrier(jnp.max(chosen, axis=1, keepdims=True)))
    gates = weights / lax.optimization_barrier(jnp.sum(weights, axis=1, keepdims=True))
    padded = jnp.concatenate([low(normed_two), jnp.zeros((1, D), jnp.float32)], axis=0)
    rows = low_back(padded[owner_row // 2])
    return (hidden, gates, rows)

def expert_apply(operands):
    rows, w_in_one, w_out_one = operands
    pre = low_back(jnp.dot(rows, w_in_one.T, precision=highest))
    act = low(jax.nn.gelu(pre))
    return low(low_back(jnp.dot(act, w_out_one, precision=highest)))

def pick_rows(table, spots):
    return table[spots]

def reference(tokens, lengths, routes, gain_one, w_query, w_key, w_value, w_attn_out, gain_two, w_gate, frozen_in, frozen_out, new_in, new_out, out_grad):
    x_rows = tokens.astype(jnp.float32).reshape(SEQS, SEQ, D)
    route_rows = routes.astype(jnp.int32).reshape(SEQS, SEQ, 2)
    length_rows = lengths.astype(jnp.int32)
    spots, owners = jax.vmap(partial(slot_tables, experts=EXPERTS, capacity=CAP, seq_len=SEQ))(route_rows)
    frozen_in_f = frozen_in.astype(jnp.float32)
    frozen_out_f = frozen_out.astype(jnp.float32)

    def forward(x_all, gain_a, query_w, key_w, value_w, attn_w, gain_b, gate_w, new_in_w, new_out_w):

        def one_block(operands):
            x_row, length_row, route_row, owner_row = operands
            return front_block(x_row, length_row, route_row, owner_row, gain_a, query_w, key_w, value_w, attn_w, gain_b, gate_w)
        hidden, gates, rows = lax.map(jax.checkpoint(one_block), (x_all, length_rows, route_rows, owners))
        by_expert = rows.reshape(SEQS, EXPERTS, CAP, D).transpose(1, 0, 2, 3).reshape(EXPERTS, SEQS * CAP, D)
        w_in_all = jnp.concatenate([frozen_in_f, new_in_w], axis=0)
        w_out_all = jnp.concatenate([frozen_out_f, new_out_w], axis=0)
        produced = lax.map(jax.checkpoint(expert_apply), (by_expert, w_in_all, w_out_all))
        per_seq = produced.reshape(EXPERTS, SEQS, CAP, D).transpose(1, 0, 2, 3).reshape(SEQS, EXPERTS * CAP, D)
        picked = jax.vmap(pick_rows)(per_seq, spots).reshape(SEQS, SEQ, 2, D)
        return hidden + lax.optimization_barrier(jnp.sum(gates[..., None] * picked, axis=2))
    primals = (x_rows, gain_one, w_query.astype(jnp.float32), w_key.astype(jnp.float32), w_value.astype(jnp.float32), w_attn_out.astype(jnp.float32), gain_two, w_gate, new_in.astype(jnp.float32), new_out.astype(jnp.float32))
    final, pull = jax.vjp(forward, *primals)
    grads = pull(out_grad.astype(jnp.float32).reshape(SEQS, SEQ, D))
    return (final.reshape(TOKENS, D).astype(jnp.bfloat16), grads[0].reshape(TOKENS, D), grads[1], grads[2], grads[3], grads[4], grads[5], grads[6], grads[7], grads[8], grads[9])
```

```python
import functools

import jax
import jax.numpy as jnp
from jax import lax
from jax.experimental import pallas as pl
from jax.experimental.pallas import tpu as pltpu
from jax.sharding import PartitionSpec as P

HEADS = 12
WINDOW = 512
F32 = jnp.float32
BF16 = jnp.bfloat16


highest = lax.Precision.HIGHEST
epsilon = 1e-05


def nt_dot(a, b):
    return lax.dot_general(a, b, (((1,), (1,)), ((), ())), preferred_element_type=F32)


def dot(a, b):
    return jnp.dot(a, b, preferred_element_type=F32)


def key_start(q_from, window):
    return max(0, q_from - window)


def fill_bias(first_ref, bias_ref, seq, block, window):
    for q_from in range(0, seq, block):
        low = key_start(q_from, window)
        size = q_from + block - low
        key = lax.broadcasted_iota(jnp.int32, (size, block), 0) + low
        place = lax.broadcasted_iota(jnp.int32, (size, block), 1) + q_from
        first = first_ref[0:1, q_from : q_from + block]
        keep = (key >= first) & (key <= place)
        bias_ref[0:size, q_from : q_from + block] = jnp.where(keep, 0.0, -1e9)


def attend_kernel(first_ref, q_ref, k_ref, v_ref, o_ref, lse_ref, bias_ref, vt_ref, ot_ref, *, block, window, scale):
    seq = q_ref.shape[0]
    half = q_ref.shape[1] // 2

    @pl.when(pl.program_id(0) == 0)
    def _():
        fill_bias(first_ref, bias_ref, seq, block, window)

    vt_ref[...] = v_ref[...].T
    lane = lax.broadcasted_iota(jnp.int32, (block, 2 * half), 1)
    for q_from in range(0, seq, block):
        low = key_start(q_from, window)
        high = q_from + block
        q_both = q_ref[q_from:high, :] * scale
        for head in range(2):
            q_one = jnp.where((lane < half) == (head == 0), q_both, jnp.zeros_like(q_both))
            scores = nt_dot(k_ref[low:high, :], q_one) + bias_ref[0 : high - low, q_from:high]
            top = jnp.max(scores, axis=0, keepdims=True)
            expd = jnp.exp(scores - top)
            total = jnp.sum(expd, axis=0, keepdims=True)
            mixed = dot(vt_ref[head * half : (head + 1) * half, low:high], expd.astype(BF16))
            ot_ref[head * half : (head + 1) * half, q_from:high] = mixed / total
            lse_ref[0, head : head + 1, q_from:high] = top + jnp.log(total)
    o_ref[...] = ot_ref[...].T.astype(BF16)


def attend(first, q, k, v, heads, window, block=256):
    seq, width = q.shape
    pair = 2 * width // heads
    col = pl.BlockSpec((seq, pair), lambda i: (0, i))
    return pl.pallas_call(
        functools.partial(attend_kernel, block=block, window=window, scale=(width // heads) ** -0.5),
        grid=(heads // 2,),
        in_specs=[pl.BlockSpec((1, seq), lambda i: (0, 0)), col, col, col],
        out_specs=[col, pl.BlockSpec((1, 8, seq), lambda i: (i, 0, 0))],
        out_shape=[
            jax.ShapeDtypeStruct((seq, width), BF16),
            jax.ShapeDtypeStruct((heads // 2, 8, seq), F32),
        ],
        scratch_shapes=[
            pltpu.VMEM((window + block, seq), F32),
            pltpu.VMEM((pair, seq), BF16),
            pltpu.VMEM((pair, seq), F32),
        ],
        compiler_params=pltpu.CompilerParams(vmem_limit_bytes=48 << 20),
        cost_estimate=pl.CostEstimate(flops=8 * seq * seq * width, bytes_accessed=8 * seq * width, transcendentals=seq * seq * heads),
        name="attend",
    )(first, q, k, v)


def attend_back_kernel(first_ref, lse_ref, q_ref, k_ref, v_ref, o_ref, do_ref, dq_ref, dk_ref, dv_ref, bias_ref, kt_ref, dqt_ref, delta_ref, dk_acc, dv_acc, *, block, window, scale):
    seq = q_ref.shape[0]
    half = q_ref.shape[1] // 2

    @pl.when(pl.program_id(0) == 0)
    def _():
        fill_bias(first_ref, bias_ref, seq, block, window)

    kt_ref[...] = k_ref[...].T
    both = (o_ref[...].astype(F32) * do_ref[...].astype(F32)).T
    delta_ref[0:1, :] = jnp.sum(both[0:half], axis=0, keepdims=True)
    delta_ref[1:2, :] = jnp.sum(both[half:], axis=0, keepdims=True)
    lane = lax.broadcasted_iota(jnp.int32, (block, 2 * half), 1)
    dk_acc[...] = jnp.zeros_like(dk_acc)
    dv_acc[...] = jnp.zeros_like(dv_acc)
    for q_from in range(0, seq, block):
        low = key_start(q_from, window)
        high = q_from + block
        q_both = q_ref[q_from:high, :] * scale
        do_both = do_ref[q_from:high, :]
        for head in range(2):
            mine = (lane < half) == (head == 0)
            q_one = jnp.where(mine, q_both, jnp.zeros_like(q_both))
            do_one = jnp.where(mine, do_both, jnp.zeros_like(do_both))
            scores = nt_dot(k_ref[low:high, :], q_one) + bias_ref[0 : high - low, q_from:high]
            probs = jnp.exp(scores - lse_ref[0, head : head + 1, q_from:high])
            prob_grad = nt_dot(v_ref[low:high, :], do_one)
            dv_acc[low:high, :] += dot(probs.astype(BF16), do_one)
            score_grad = (probs * (prob_grad - delta_ref[head : head + 1, q_from:high])).astype(BF16)
            dk_acc[low:high, :] += dot(score_grad, q_one)
            dqt_ref[head * half : (head + 1) * half, q_from:high] = dot(
                kt_ref[head * half : (head + 1) * half, low:high], score_grad
            )
    dq_ref[...] = (dqt_ref[...].T * scale).astype(BF16)
    dk_ref[...] = dk_acc[...].astype(BF16)
    dv_ref[...] = dv_acc[...].astype(BF16)


def attend_back(first, lse, q, k, v, o, do, heads, window, block=256):
    seq, width = q.shape
    pair = 2 * width // heads
    col = pl.BlockSpec((seq, pair), lambda i: (0, i))
    shape = jax.ShapeDtypeStruct((seq, width), BF16)
    return pl.pallas_call(
        functools.partial(attend_back_kernel, block=block, window=window, scale=(width // heads) ** -0.5),
        grid=(heads // 2,),
        in_specs=[
            pl.BlockSpec((1, seq), lambda i: (0, 0)),
            pl.BlockSpec((1, 8, seq), lambda i: (i, 0, 0)),
            col, col, col, col, col,
        ],
        out_specs=[col, col, col],
        out_shape=[shape, shape, shape],
        scratch_shapes=[
            pltpu.VMEM((window + block, seq), F32),
            pltpu.VMEM((pair, seq), BF16),
            pltpu.VMEM((pair, seq), F32),
            pltpu.VMEM((8, seq), F32),
            pltpu.VMEM((seq, pair), F32),
            pltpu.VMEM((seq, pair), F32),
        ],
        compiler_params=pltpu.CompilerParams(vmem_limit_bytes=48 << 20),
        cost_estimate=pl.CostEstimate(flops=20 * seq * seq * width, bytes_accessed=16 * seq * width, transcendentals=seq * seq * heads),
        name="attend_back",
    )(first, lse, q, k, v, o, do)


def gather_kernel(spots_ref, gates_ref, source_ref, rows_ref, *, first, capacity, gated):
    rows = rows_ref.shape[1]
    seq = source_ref.shape[0]
    slot = lax.broadcasted_iota(jnp.int32, (rows, seq), 0)
    slot = slot + (pl.program_id(0) + first) * capacity
    zero = slot == spots_ref[0:1, :]
    one = slot == spots_ref[1:2, :]
    taken = dot((zero | one).astype(BF16), source_ref[...])
    if gated:
        weight = jnp.where(zero, gates_ref[0:1, :], 0.0) + jnp.where(one, gates_ref[1:2, :], 0.0)
        taken = taken * jnp.sum(weight, axis=1, keepdims=True)
    rows_ref[0] = taken.astype(BF16)


def gather_rows(spots, gates, source, first, count, capacity, gated):
    seq, width = source.shape
    fixed = lambda i: (0, 0)
    return pl.pallas_call(
        functools.partial(gather_kernel, first=first, capacity=capacity, gated=gated),
        grid=(count,),
        in_specs=[
            pl.BlockSpec((2, seq), fixed),
            pl.BlockSpec((2, seq), fixed),
            pl.BlockSpec((seq, width), fixed),
        ],
        out_specs=pl.BlockSpec((1, capacity, width), lambda i: (i, 0, 0)),
        out_shape=jax.ShapeDtypeStruct((count, capacity, width), BF16),
        compiler_params=pltpu.CompilerParams(vmem_limit_bytes=40 << 20),
        cost_estimate=pl.CostEstimate(
            flops=2 * count * capacity * seq * width,
            bytes_accessed=2 * (count * capacity + seq) * width,
            transcendentals=0,
        ),
        name="gather_rows",
    )(spots, gates, source)


def normal_of(hidden):
    centre = hidden - jnp.mean(hidden, axis=-1, keepdims=True)
    inverse = lax.rsqrt(jnp.mean(centre * centre, axis=-1, keepdims=True) + epsilon)
    return centre * inverse, inverse


def pick_matrix(spot, first, rows):
    slot = lax.broadcasted_iota(jnp.int32, (spot.shape[0], rows), 1) + first
    return slot == spot


def combine_kernel(spots_ref, gates_ref, routes_ref, hidden_ref, dy_ref, gain_ref, frozen_ref, new_ref, out_ref, full_ref, gate_grad_ref, *, experts):
    frozen_rows, new_rows = frozen_ref.shape[0], new_ref.shape[0]
    hidden = hidden_ref[...]
    dy = dy_ref[...].astype(F32)
    picked = []
    terms = []
    for k in range(2):
        spot = spots_ref[:, k : k + 1]
        value = dot(pick_matrix(spot, 0, frozen_rows).astype(BF16), frozen_ref[...]) + dot(
            pick_matrix(spot, frozen_rows, new_rows).astype(BF16), new_ref[...]
        )
        picked.append(value)
        terms.append(jnp.sum(value * dy, axis=1, keepdims=True))
    gates = [gates_ref[:, k : k + 1] for k in range(2)]
    out_ref[...] = (hidden + (gates[0] * picked[0] + gates[1] * picked[1])).astype(BF16)
    inner = gates[0] * terms[0] + gates[1] * terms[1]
    expert = lax.broadcasted_iota(jnp.int32, (hidden.shape[0], experts), 1)
    full = jnp.zeros(expert.shape, F32)
    for k in range(2):
        full = full + jnp.where(expert == routes_ref[:, k : k + 1], gates[k] * (terms[k] - inner), 0.0)
    full_ref[...] = full
    norm_two = normal_of(hidden)[0] * gain_ref[...]

    @pl.when(pl.program_id(0) == 0)
    def _():
        gate_grad_ref[...] = jnp.zeros_like(gate_grad_ref)

    for e in range(experts):
        gate_grad_ref[e : e + 1, :] += jnp.sum(norm_two * full[:, e : e + 1], axis=0, keepdims=True)


def combine(spots, gates, routes, hidden, dy, gain, frozen_out, new_out, experts, block=256):
    seq, width = hidden.shape
    fixed = lambda i: (0, 0)
    moving = lambda i: (i, 0)
    return pl.pallas_call(
        functools.partial(combine_kernel, experts=experts),
        grid=(seq // block,),
        in_specs=[
            pl.BlockSpec((block, 2), moving),
            pl.BlockSpec((block, 2), moving),
            pl.BlockSpec((block, 2), moving),
            pl.BlockSpec((block, width), moving),
            pl.BlockSpec((block, width), moving),
            pl.BlockSpec((1, width), fixed),
            pl.BlockSpec(frozen_out.shape, fixed),
            pl.BlockSpec(new_out.shape, fixed),
        ],
        out_specs=[
            pl.BlockSpec((block, width), moving),
            pl.BlockSpec((block, experts), moving),
            pl.BlockSpec((experts, width), fixed),
        ],
        out_shape=[
            jax.ShapeDtypeStruct((seq, width), BF16),
            jax.ShapeDtypeStruct((seq, experts), F32),
            jax.ShapeDtypeStruct((experts, width), F32),
        ],
        compiler_params=pltpu.CompilerParams(vmem_limit_bytes=48 << 20),
        cost_estimate=pl.CostEstimate(
            flops=4 * seq * (frozen_out.shape[0] + new_out.shape[0]) * width,
            bytes_accessed=16 * seq * width,
            transcendentals=0,
        ),
        name="combine",
    )(spots, gates, routes, hidden, dy, gain, frozen_out, new_out)


def combine_back_kernel(spots_ref, full_ref, hidden_ref, dy_ref, gain_ref, w_gate_ref, frozen_ref, new_ref, grad_ref, branch_ref, gain_grad_ref):
    frozen_rows, new_rows = frozen_ref.shape[0], new_ref.shape[0]
    spot_zero, spot_one = spots_ref[:, 0:1], spots_ref[:, 1:2]

    def both(first, rows):
        return (pick_matrix(spot_zero, first, rows) | pick_matrix(spot_one, first, rows)).astype(BF16)

    upstream = dot(both(0, frozen_rows), frozen_ref[...]) + dot(both(frozen_rows, new_rows), new_ref[...])
    full = full_ref[...]
    for e in range(w_gate_ref.shape[0]):
        upstream = upstream + full[:, e : e + 1] * w_gate_ref[e : e + 1, :]
    normal, inverse = normal_of(hidden_ref[...])

    @pl.when(pl.program_id(0) == 0)
    def _():
        gain_grad_ref[...] = jnp.zeros_like(gain_grad_ref)

    gain_grad_ref[...] += jnp.sum(upstream * normal, axis=0, keepdims=True)
    scaled = upstream * gain_ref[...]
    inner = (
        scaled
        - jnp.mean(scaled, axis=-1, keepdims=True)
        - normal * jnp.mean(scaled * normal, axis=-1, keepdims=True)
    )
    grad = dy_ref[...].astype(F32) + inner * inverse
    grad_ref[...] = grad
    branch_ref[...] = grad.astype(BF16)


def combine_back(spots, full, hidden, dy, gain, w_gate_t, frozen_back, new_back, block=256):
    seq, width = hidden.shape
    experts = w_gate_t.shape[0]
    fixed = lambda i: (0, 0)
    moving = lambda i: (i, 0)
    return pl.pallas_call(
        combine_back_kernel,
        grid=(seq // block,),
        in_specs=[
            pl.BlockSpec((block, 2), moving),
            pl.BlockSpec((block, experts), moving),
            pl.BlockSpec((block, width), moving),
            pl.BlockSpec((block, width), moving),
            pl.BlockSpec((1, width), fixed),
            pl.BlockSpec((experts, width), fixed),
            pl.BlockSpec(frozen_back.shape, fixed),
            pl.BlockSpec(new_back.shape, fixed),
        ],
        out_specs=[
            pl.BlockSpec((block, width), moving),
            pl.BlockSpec((block, width), moving),
            pl.BlockSpec((1, width), fixed),
        ],
        out_shape=[
            jax.ShapeDtypeStruct((seq, width), F32),
            jax.ShapeDtypeStruct((seq, width), BF16),
            jax.ShapeDtypeStruct((1, width), F32),
        ],
        compiler_params=pltpu.CompilerParams(vmem_limit_bytes=48 << 20),
        cost_estimate=pl.CostEstimate(
            flops=2 * seq * (frozen_back.shape[0] + new_back.shape[0]) * width,
            bytes_accessed=16 * seq * width,
            transcendentals=0,
        ),
        name="combine_back",
    )(spots, full, hidden, dy, gain, w_gate_t, frozen_back, new_back)


def norm_backward(upstream, gain, normal_part, scale_inv):
    scaled = upstream * gain
    inner = (
        scaled
        - jnp.mean(scaled, axis=-1, keepdims=True)
        - normal_part * jnp.mean(scaled * normal_part, axis=-1, keepdims=True)
    )
    return inner * scale_inv


def first_keys(length_row, seq_len):
    ends = jnp.cumsum(length_row)
    places = jnp.arange(seq_len, dtype=jnp.int32)
    passed = places[None, :] >= ends[:, None]
    return jnp.max(jnp.where(passed, ends[:, None], 0), axis=0, keepdims=True)


def slot_spots(routes, experts, capacity):
    names = jnp.arange(experts, dtype=jnp.int32)[None, :]
    zero, one = routes[:, 0:1] == names, routes[:, 1:2] == names
    picks = (zero | one).astype(jnp.int32)
    earlier = jnp.cumsum(picks, axis=0) - picks
    ranks = [jnp.sum(jnp.where(mine, earlier, 0), axis=1, keepdims=True) for mine in (zero, one)]
    return routes * capacity + jnp.concatenate(ranks, axis=1), zero, one


def gelu_grad(pre, upstream):
    return jax.vjp(jax.nn.gelu, pre)[1](upstream)[0]


def expert_forward(rows, w_in_full, w_out_full):
    pre = jnp.einsum("rd,fd->rf", rows, w_in_full, preferred_element_type=F32)
    act = jax.nn.gelu(pre).astype(BF16)
    return dot(act, w_out_full).astype(BF16), pre, act


def expert_backward(grads, pre, w_in_full, w_out_full):
    act_grad = jnp.einsum("rd,fd->rf", grads, w_out_full, preferred_element_type=F32)
    pre_grad = gelu_grad(pre, act_grad).astype(BF16)
    return dot(pre_grad, w_in_full).astype(BF16), pre_grad


def transposed_dot(a, b):
    return jnp.einsum("td,te->de", a, b, preferred_element_type=F32)


def on_device(
    tokens,
    lengths,
    routes,
    gain_one,
    w_query,
    w_key,
    w_value,
    w_attn_out,
    gain_two,
    w_gate,
    frozen_in,
    frozen_out,
    new_in,
    new_out,
    out_grad,
):
    seq_len, width = tokens.shape
    experts = w_gate.shape[1]
    frozen = frozen_in.shape[0]
    new = experts - frozen
    capacity = -(-max(2, 3 * seq_len // experts) // 8) * 8
    exchange = functools.partial(
        lax.all_to_all, axis_name="expert", split_axis=0, concat_axis=0, tiled=True
    )
    w_in = lax.all_gather(new_in, "dp", axis=1, tiled=True)[0]
    w_out = lax.all_gather(new_out, "dp", axis=1, tiled=True)[0]

    x_in = tokens.astype(F32)
    normal_one, inv_one = normal_of(x_in)
    normed = (normal_one * gain_one).astype(BF16)
    query, keys, values = [dot(normed, w).astype(BF16) for w in (w_query, w_key, w_value)]
    first = first_keys(lengths[0], seq_len)
    mixed, log_totals = attend(first, query, keys, values, HEADS, WINDOW)
    hidden = x_in + dot(mixed, w_attn_out)
    norm_two = normal_of(hidden)[0] * gain_two
    norm_low = norm_two.astype(BF16)
    spots, zero, one = slot_spots(routes, experts, capacity)
    spots_row = spots.T
    rows_new = gather_rows(
        spots_row, jnp.zeros((2, seq_len), F32), norm_low, frozen, new, capacity, False
    )
    arrived = exchange(rows_new).reshape(-1, width)

    logits = jnp.dot(norm_two, w_gate, precision=highest)
    chosen = jnp.concatenate(
        [jnp.sum(jnp.where(mine, logits, 0.0), axis=1, keepdims=True) for mine in (zero, one)],
        axis=1,
    )
    weights = jnp.exp(chosen - jnp.max(chosen, axis=1, keepdims=True))
    gates = weights / jnp.sum(weights, axis=1, keepdims=True)
    gates_row = gates.T
    grads_new = gather_rows(spots_row, gates_row, out_grad, frozen, new, capacity, True)
    arrived_grads = exchange(grads_new).reshape(-1, width)
    rows_frozen = gather_rows(spots_row, gates_row, norm_low, 0, frozen, capacity, False)
    grads_frozen = gather_rows(spots_row, gates_row, out_grad, 0, frozen, capacity, True)
    frozen_outputs, frozen_back = [], []
    for e in range(frozen):
        produced, pre, _ = expert_forward(rows_frozen[e], frozen_in[e], frozen_out[e])
        back, _ = expert_backward(grads_frozen[e], pre, frozen_in[e], frozen_out[e])
        frozen_outputs.append(produced)
        frozen_back.append(back)
    frozen_outputs = jnp.concatenate(frozen_outputs, axis=0)
    frozen_back = jnp.concatenate(frozen_back, axis=0)

    produced, pre, act = expert_forward(arrived, w_in, w_out)
    returned = exchange(produced.reshape(new, capacity, width)).reshape(-1, width)
    rows_back, pre_grad = expert_backward(arrived_grads, pre, w_in, w_out)
    returned_back = exchange(rows_back.reshape(new, capacity, width)).reshape(-1, width)
    w_in_grad = jnp.einsum("rf,rd->fd", pre_grad, arrived, preferred_element_type=F32)
    w_out_grad = jnp.einsum("rf,rd->fd", act, arrived_grads, preferred_element_type=F32)
    new_in_grad = lax.psum_scatter(
        w_in_grad.astype(BF16)[None], "dp", scatter_dimension=1, tiled=True
    )
    new_out_grad = lax.psum_scatter(
        w_out_grad.astype(BF16)[None], "dp", scatter_dimension=1, tiled=True
    )

    output, full_logit_grad, w_gate_grad = combine(
        spots, gates, routes, hidden, out_grad, gain_two[None], frozen_outputs, returned, experts
    )
    hidden_grad, branch_grad, gain_two_grad = combine_back(
        spots, full_logit_grad, hidden, out_grad, gain_two[None], w_gate.T, frozen_back, returned_back
    )
    mixed_grad = jnp.einsum("te,de->td", branch_grad, w_attn_out, preferred_element_type=F32)
    w_attn_out_grad = transposed_dot(mixed, branch_grad)
    small = -(-(experts + 1) // 16) * 16
    early = jnp.concatenate(
        [
            w_attn_out_grad,
            w_gate_grad,
            gain_two_grad,
            jnp.zeros((small - experts - 1, width), F32),
        ],
        axis=0,
    ).astype(BF16)
    early = lax.psum(early, ("dp", "expert"))
    query_grad, key_grad, value_grad = attend_back(
        first, log_totals, query, keys, values, mixed, mixed_grad.astype(BF16), HEADS, WINDOW
    )
    late = jnp.concatenate(
        [transposed_dot(normed, g) for g in (query_grad, key_grad, value_grad)], axis=0
    ).astype(BF16)
    late, early = lax.optimization_barrier((late, early))
    late = lax.psum(late, ("dp", "expert")).astype(F32).reshape(3, width, width)
    early = early.astype(F32)
    normed_grad = sum(
        jnp.einsum("te,de->td", g, w, preferred_element_type=F32)
        for g, w in ((query_grad, w_query), (key_grad, w_key), (value_grad, w_value))
    )
    x_grad = hidden_grad + norm_backward(normed_grad, gain_one, normal_one, inv_one)
    gain_one_grad = (
        sum(
            jnp.sum(late[i] * w.astype(F32), axis=1)
            for i, w in enumerate((w_query, w_key, w_value))
        )
        / gain_one
    )
    return (
        output,
        x_grad,
        gain_one_grad,
        late[0],
        late[1],
        late[2],
        early[:width],
        early[width + experts],
        early[width : width + experts].T,
        new_in_grad.astype(F32),
        new_out_grad.astype(F32),
    )


def solution(mesh):
    return jax.shard_map(
        on_device,
        mesh=mesh,
        in_specs=(
            P(("dp", "expert"), None),
            P(("dp", "expert"), None),
            P(("dp", "expert"), None),
            P(),
            P(),
            P(),
            P(),
            P(),
            P(),
            P(),
            P(),
            P(),
            P("expert", "dp", None),
            P("expert", "dp", None),
            P(("dp", "expert"), None),
        ),
        out_specs=(
            P(("dp", "expert"), None),
            P(("dp", "expert"), None),
            P(),
            P(),
            P(),
            P(),
            P(),
            P(),
            P(),
            P("expert", "dp", None),
            P("expert", "dp", None),
        ),
        check_vma=False,
    )
```
